32 devices in a mesh: ta: 2 (over x), gz: 4 (over y, core), gy: 4 (over z).
Axes of the slice: x: 2, y: 2, z: 4, core: 2. Of those that a mesh axis runs over, the one named last changes fastest.
Arguments:
- propagator: bfloat16 [2, 4, 3, 12, 2, 4, 512], P(None, None, None, None, 'ta', 'gz', 'gy'), may hold values from -6 to 6
- links: bfloat16 [2, 3, 3, 2, 4, 512], P(None, None, None, 'ta', 'gz', 'gy'), may hold values from -2.5 to 2.5
- source_z: int32 [2, 4], replicated, may hold values from 0 to 3
- displacements: int32 [3], replicated, may hold values from 0 to 2, each once
- momenta: int32 [4], replicated, may hold values from 1 to 3
- gamma_perm: int32 [4, 4], replicated, may hold values from 0 to 3, each once within a row
- gamma_phase: int32 [4, 4], replicated, may hold values from 0 to 3
Outputs:
- correlator: float32 [2, 3, 4, 4, 2], replicated
The draws below stay inside these ranges and needn't reach their ends.
Inputs may be any that keep to these rules, and one draw needn't show every extreme that they name: `displacements`: every displacement from -1 to 1 appears exactly once. `gamma_perm`: each row is a permutation of the four spin indices.
All inputs are finite; a program needn't handle non-finite values.
Results may differ from the reference program's by a relative error of at most 0.0003.
Values may be sent and summed in bfloat16 or wider, within the bound.
A program may use at most 64 MiB of HBM per device.

```python
import math
import jax
import jax.numpy as jnp
from jax import lax

NX = 64
NG = 4
NP = 4
NSTEP = 1
NDISP = 3
NT = 2
NZ = 4
NY = 8
NYX = 512


def with_ends(array, rng, least, largest):
    longest = array.shape.index(max(array.shape))
    spots = []
    for shift in (0, 1):
        where = [jax.random.randint(jax.random.fold_in(rng, axis), (), 0, length) for axis, length in enumerate(array.shape)]
        where[longest] = (where[longest] + shift) % array.shape[longest]
        spots.append(tuple(where))
    return array.at[spots[0]].set(least).at[spots[1]].set(largest)


def block_levels(rng, dims, shards, least, high):
    level, own = 1.0, jax.random.fold_in(rng, 6)
    for axis_at, blocks in shards:
        steps = jnp.exp(jax.random.uniform(jax.random.fold_in(own, axis_at), (blocks,), jnp.float32, least / len(shards), high / len(shards)))
        level = level * jnp.repeat(steps, dims[axis_at] // blocks).reshape([-1 if axis == axis_at else 1 for axis in range(len(dims))])
    return level


def centred(own_key, extent, width, most, split=(), held_as=jnp.bfloat16):
    gain = block_levels(own_key, extent, split, -0.22, 0.18) if split else 1.0
    array = jax.random.normal(own_key, extent, jnp.float32) * width * gain
    return jnp.minimum(jnp.maximum(array, -most), most).astype(held_as)


def setup_inputs(seed: int = 0) -> dict:
    key_of = jax.random.split(jax.random.key(seed), 8)
    return {
        "propagator": centred(key_of[0], (2, 4, 3, 12, NT, NZ, NYX), 1.0, 6.0, ((4, 2), (5, 4), (6, 4))),
        "links": centred(key_of[1], (2, 3, 3, NT, NZ, NYX), 6 ** -0.5, 2.5, ((3, 2), (4, 4), (5, 4))),
        "source_z": with_ends(jax.random.randint(key_of[2], (NT, NP), 0, NZ), jax.random.fold_in(key_of[2], 1), 0, NZ - 1).astype(jnp.int32),
        "displacements": jax.random.permutation(key_of[3], NDISP).astype(jnp.int32),
        "momenta": with_ends(jax.random.randint(key_of[4], (NP,), 1, 4), jax.random.fold_in(key_of[4], 1), 1, 3).astype(jnp.int32),
        "gamma_perm": jax.vmap(lambda own: jax.random.permutation(own, 4))(jax.random.split(key_of[5], NG)).reshape((NG, 4)).astype(jnp.int32),
        "gamma_phase": with_ends(jax.random.randint(key_of[6], (NG, 4), 0, 4), jax.random.fold_in(key_of[6], 1), 0, 3).astype(jnp.int32),
    }


highest = lax.Precision.HIGHEST

def colour_apply(wilson, field_now):
    form = 'ab...,sbc...->sac...'
    real_part = jnp.einsum(form, wilson[0], field_now[0], precision=highest) - jnp.einsum(form, wilson[1], field_now[1], precision=highest)
    imag_part = jnp.einsum(form, wilson[0], field_now[1], precision=highest) + jnp.einsum(form, wilson[1], field_now[0], precision=highest)
    return jnp.stack([real_part, imag_part])

def link_product(left_link, right_link):
    form = 'ab...,bc...->ac...'
    real_part = jnp.einsum(form, left_link[0], right_link[0], precision=highest) - jnp.einsum(form, left_link[1], right_link[1], precision=highest)
    imag_part = jnp.einsum(form, left_link[0], right_link[1], precision=highest) + jnp.einsum(form, left_link[1], right_link[0], precision=highest)
    return jnp.stack([real_part, imag_part])

def dagger(link_field):
    return jnp.stack([jnp.swapaxes(link_field[0], 0, 1), -jnp.swapaxes(link_field[1], 0, 1)])

def spin_pairs(source, field_now):
    form = 'sac...,uac...->su...'
    real_part = jnp.einsum(form, source[0], field_now[0], precision=highest) + jnp.einsum(form, source[1], field_now[1], precision=highest)
    imag_part = jnp.einsum(form, source[0], field_now[1], precision=highest) - jnp.einsum(form, source[1], field_now[0], precision=highest)
    return (real_part, imag_part)

def insert(gamma_real, gamma_imag, pairs):
    pair_real, pair_imag = pairs
    form = 'gsu,su...->g...'
    real_part = jnp.einsum(form, gamma_real, pair_real, precision=highest) - jnp.einsum(form, gamma_imag, pair_imag, precision=highest)
    imag_part = jnp.einsum(form, gamma_real, pair_imag, precision=highest) + jnp.einsum(form, gamma_imag, pair_real, precision=highest)
    return (real_part, imag_part)

def gamma_tables(gamma_perm, gamma_phase):
    columns = jnp.arange(4, dtype=jnp.int32)
    hits = (gamma_perm[:, :, None] == columns[None, None, :]).astype(jnp.float32)
    real_part = (gamma_phase == 0).astype(jnp.float32) - (gamma_phase == 2).astype(jnp.float32)
    imag_part = (gamma_phase == 1).astype(jnp.float32) - (gamma_phase == 3).astype(jnp.float32)
    return (hits * real_part[:, :, None], hits * imag_part[:, :, None])

def reference(propagator, links, source_z, displacements, momenta, gamma_perm, gamma_phase):
    gamma_real, gamma_imag = gamma_tables(gamma_perm, gamma_phase)
    depth_index = jnp.arange(NZ, dtype=jnp.int32)
    turn_count = momenta[None, :, None] * (depth_index[None, None, :] - source_z[:, :, None]) % NZ
    angles = turn_count.astype(jnp.float32) * (2.0 * math.pi / NZ)
    cosine_all = jnp.cos(angles)
    sine_all = jnp.sin(angles)
    scaling = 1.0 / (24.0 * math.sqrt(NX * NY * NZ))
    unit = jnp.broadcast_to(jnp.eye(3, dtype=jnp.float32)[:, :, None, None], (3, 3, NZ, NYX))
    identity = jnp.stack([unit, jnp.zeros_like(unit)])

    def one_slice(slice_pack):
        source = slice_pack[0].astype(jnp.float32)
        link_field = slice_pack[1].astype(jnp.float32)
        cosine = slice_pack[2]
        sine_table = slice_pack[3]

        def project(field_now):
            trace_real, trace_imag = insert(gamma_real, gamma_imag, spin_pairs(source, field_now))
            line_real = lax.optimization_barrier(jnp.sum(trace_real, axis=-1))
            line_imag = lax.optimization_barrier(jnp.sum(trace_imag, axis=-1))
            real_part = jnp.dot(line_real, cosine.T, precision=highest) + jnp.dot(line_imag, sine_table.T, precision=highest)
            imag_part = jnp.dot(line_imag, cosine.T, precision=highest) - jnp.dot(line_real, sine_table.T, precision=highest)
            return jnp.stack([real_part, imag_part], axis=-1) * scaling
        results = {0: project(source)}
        wilson = identity
        for reach in range(1, NSTEP + 1):
            wilson = link_product(wilson, jnp.roll(link_field, -(reach - 1), axis=3))
            results[reach] = project(colour_apply(wilson, jnp.roll(source, -reach, axis=4)))
        wilson = identity
        for reach in range(1, NSTEP + 1):
            wilson = link_product(wilson, dagger(jnp.roll(link_field, reach, axis=3)))
            results[-reach] = project(colour_apply(wilson, jnp.roll(source, reach, axis=4)))
        return jnp.stack([results[offset] for offset in range(-NSTEP, NSTEP + 1)])
    slices = lax.map(one_slice, (jnp.moveaxis(propagator, 4, 0), jnp.moveaxis(links, 3, 0), cosine_all, sine_all))
    return jnp.take(slices, displacements.astype(jnp.int32), axis=1)
```

```python
import functools
import math

import jax
import jax.numpy as jnp
from jax import lax
from jax.experimental import pallas as pl
from jax.experimental.pallas import tpu as pltpu
from jax.sharding import PartitionSpec as P

MESH = pl.DeviceIdType.MESH
LANES = 128


def weights(lane_row, sizes, smem, place, scaling):
    ndisp, ng, np_, nz = sizes
    src, disp, mom, perm, phase = smem
    slice_at, depth_at = place
    nsteps = (ndisp - 1) // 2
    shape = (32, LANES)
    lane = lax.broadcasted_iota(jnp.int32, shape, 1) + lane_row * LANES
    row = lax.broadcasted_iota(jnp.int32, shape, 0)
    momentum = lane & (np_ - 1)
    out_part = (lane // np_) & 1
    gamma = (lane // (2 * np_)) & (ng - 1)
    entry = lane // (2 * np_ * ng)
    in_part = row // 16
    first = (row // 4) & 3
    second = row & 3
    reach = jnp.full(shape, 2 * nsteps + 1, jnp.int32)
    for j in range(ndisp):
        reach = jnp.where(entry == j, disp[j] - nsteps, reach)
    backward = reach < 0
    momenta = jnp.zeros(shape, jnp.int32)
    source = jnp.zeros(shape, jnp.int32)
    for p in range(np_):
        momenta = jnp.where(momentum == p, mom[p], momenta)
        source = jnp.where(momentum == p, src[slice_at, p], source)
    depth = depth_at - jnp.where(backward, reach, 0)
    turns = (momenta * (depth - source)).astype(jnp.float32) * (1.0 / nz)
    angle = (turns - jnp.floor(turns)) * (2.0 * math.pi)
    cosine = jnp.cos(angle)
    sine = jnp.sin(angle)
    sink = jnp.where(backward, second, first)
    other = jnp.where(backward, first, second)
    column = jnp.zeros(shape, jnp.int32)
    power = jnp.zeros(shape, jnp.int32)
    for g in range(ng):
        for s in range(4):
            here = (gamma == g) & (sink == s)
            column = jnp.where(here, perm[g, s], column)
            power = jnp.where(here, phase[g, s], power)
    quarter = power - out_part + jnp.where(backward, -in_part, in_part)
    quarter = quarter & 3
    value = jnp.where((quarter & 1) == 0, cosine, sine)
    value = jnp.where(quarter >= 2, -value, value)
    value = jnp.where((column == other) & (entry < ndisp), value * scaling, 0.0)
    return value, jnp.abs(reach)


def pair_sums(left, right, rows):
    half = rows // 2
    per = half // 4
    lefts = []
    turned = []
    rights = []
    for s in range(4):
        lefts.append(left[pl.ds(s, 2 * per, stride=4), :])
        rights.append(right[pl.ds(s, 2 * per, stride=4), :])
        turned.append(
            jnp.concatenate(
                [-left[pl.ds(half + s, per, stride=4), :], left[pl.ds(s, per, stride=4), :]],
                axis=0,
            )
        )
    out = []
    for group in (lefts, turned):
        for s in range(4):
            for u in range(4):
                product = (group[s] * rights[u]).reshape(2 * per // 8, 8, LANES)
                out.append(jnp.sum(jnp.sum(product, axis=0), axis=0, keepdims=True))
    stacked = jnp.concatenate(out, axis=0)
    return jnp.sum(stacked, axis=1, keepdims=True)


def kernel(
    sizes, scaling, ranks,
    prop, links, src_h, disp_h, mom_h, perm_h, phase_h,
    out,
    near, near_links, far, far_links, left, right,
    src, disp, mom, perm, phase,
    stage1, stage2,
    local_sem, s_send, s_recv, u_send, u_recv, a_send, a_recv, b_send, b_recv,
):
    ndisp, ng, np_, nz = sizes
    nta, ngz, ngy = ranks
    nsteps = (ndisp - 1) // 2
    rows = near.shape[0]
    part_rows = rows // 2
    colour_rows = part_rows // 3
    lane_rows = stage1.shape[1]
    ta, gz, gy = lax.axis_index("ta"), lax.axis_index("gz"), lax.axis_index("gy")

    loads = [
        pltpu.make_async_copy(a, b, local_sem.at[i])
        for i, (a, b) in enumerate(
            [(prop, near), (links, near_links), (src_h, src), (disp_h, disp),
             (mom_h, mom), (perm_h, perm), (phase_h, phase)]
        )
    ]
    for load in loads:
        load.start()

    barrier = pltpu.get_barrier_semaphore()
    peers1 = [(ta, lax.rem(gz + d, ngz), gy) for d in range(1, ngz)]
    peers2 = [
        (lax.rem(ta + i, nta), gz, lax.rem(gy + j, ngy))
        for i in range(nta) for j in range(ngy) if i + j
    ]
    for peer in peers1 + peers2:
        pl.semaphore_signal(barrier, inc=1, device_id=peer, device_id_type=MESH)
    pl.semaphore_wait(barrier, len(peers1) + len(peers2))

    loads[0].wait()
    loads[1].wait()
    sends = []
    for k in range(1, nsteps + 1):
        target = (ta, lax.rem(gz + ngz - k, ngz), gy)
        sends.append(pltpu.make_async_remote_copy(
            src_ref=near, dst_ref=far.at[k - 1], send_sem=s_send.at[k - 1],
            recv_sem=s_recv.at[k - 1], device_id=target, device_id_type=MESH))
        sends[-1].start()
    link_sends = []
    for k in range(1, nsteps):
        target = (ta, lax.rem(gz + ngz - k, ngz), gy)
        link_sends.append(pltpu.make_async_remote_copy(
            src_ref=near_links, dst_ref=far_links.at[k - 1], send_sem=u_send.at[k - 1],
            recv_sem=u_recv.at[k - 1], device_id=target, device_id_type=MESH))
        link_sends[-1].start()

    for load in loads[2:]:
        load.wait()
    left[...] = near[...].astype(jnp.float32)
    sums = [pair_sums(left, left, rows)]
    tables = [
        weights(h, sizes, (src, disp, mom, perm, phase), (ta, gz), scaling)
        for h in range(lane_rows)
    ]

    def link_at(ref):
        return [
            [
                [jnp.broadcast_to(ref[3 * a + b, pl.ds(part, 1), :].astype(jnp.float32), (8, LANES))
                 for part in range(2)]
                for b in range(3)
            ]
            for a in range(3)
        ]

    wilson = None
    for k in range(1, nsteps + 1):
        if k == 1:
            wilson = link_at(near_links)
        else:
            link_sends[k - 2].wait_recv()
            step = link_at(far_links.at[k - 2])
            wilson = [
                [
                    [
                        sum(wilson[a][c][0] * step[c][b][0] - wilson[a][c][1] * step[c][b][1] for c in range(3)),
                        sum(wilson[a][c][0] * step[c][b][1] + wilson[a][c][1] * step[c][b][0] for c in range(3)),
                    ]
                    for b in range(3)
                ]
                for a in range(3)
            ]
        sends[k - 1].wait_recv()
        for chunk in range(colour_rows // 16):
            field = [
                [
                    far[k - 1, pl.ds(part * part_rows + b * colour_rows + chunk * 16, 16), :]
                    .astype(jnp.float32).reshape(2, 8, LANES)
                    for b in range(3)
                ]
                for part in range(2)
            ]
            for a in range(3):
                real = sum(wilson[a][b][0] * field[0][b] - wilson[a][b][1] * field[1][b] for b in range(3))
                imag = sum(wilson[a][b][0] * field[1][b] + wilson[a][b][1] * field[0][b] for b in range(3))
                at = a * colour_rows + chunk * 16
                right[pl.ds(at, 16), :] = real.reshape(16, LANES)
                right[pl.ds(part_rows + at, 16), :] = imag.reshape(16, LANES)
        sums.append(pair_sums(left, right, rows))

    for h in range(lane_rows):
        table, reach = tables[h]
        chosen = jnp.zeros(table.shape, jnp.float32)
        for k in range(nsteps + 1):
            chosen = jnp.where(reach == k, sums[k], chosen)
        stage1[gz, pl.ds(h, 1), :] = jnp.sum(chosen * table, axis=0, keepdims=True)

    first = []
    for d in range(1, ngz):
        first.append(pltpu.make_async_remote_copy(
            src_ref=stage1.at[gz], dst_ref=stage1.at[gz], send_sem=a_send.at[d],
            recv_sem=a_recv.at[d], device_id=peers1[d - 1], device_id_type=MESH))
        first[-1].start()
    for copy in first:
        copy.wait_recv()
    total = stage1[0]
    for d in range(1, ngz):
        total = total + stage1[d]
    stage2[ta, gy] = total
    second = []
    for d, peer in enumerate(peers2):
        second.append(pltpu.make_async_remote_copy(
            src_ref=stage2.at[ta, gy], dst_ref=stage2.at[ta, gy], send_sem=b_send.at[d],
            recv_sem=b_recv.at[d], device_id=peer, device_id_type=MESH))
        second[-1].start()
    for copy in second:
        copy.wait_recv()
    for t in range(nta):
        total = stage2[t, 0]
        for d in range(1, ngy):
            total = total + stage2[t, d]
        out[t] = total
    for copy in sends + link_sends + first + second:
        copy.wait_send()


def body(ranks, propagator, links, source_z, displacements, momenta, gamma_perm, gamma_phase):
    nta, ngz, ngy = ranks
    sites = propagator.shape[6]
    ndisp, np_, ng = displacements.shape[0], momenta.shape[0], gamma_perm.shape[0]
    nsteps = (ndisp - 1) // 2
    sizes = (ndisp, ng, np_, ngz)
    scaling = 1.0 / (24.0 * math.sqrt(sites * ngy * ngz))
    field = jnp.transpose(propagator, (0, 2, 3, 4, 5, 1, 6)).reshape(-1, sites)
    link = jnp.transpose(links, (1, 2, 3, 4, 0, 5)).reshape(9, 2, sites)
    rows = field.shape[0]
    lane_rows = -(-ndisp * ng * np_ * 2 // LANES)
    more = max(nsteps - 1, 1)
    dma = pltpu.SemaphoreType.DMA
    reduced = pl.pallas_call(
        functools.partial(kernel, sizes, scaling, ranks),
        out_shape=jax.ShapeDtypeStruct((nta, lane_rows, LANES), jnp.float32),
        in_specs=[pl.BlockSpec(memory_space=pl.ANY)] * 7,
        out_specs=pl.BlockSpec(memory_space=pltpu.VMEM),
        scratch_shapes=[
            pltpu.VMEM((rows, sites), jnp.bfloat16),
            pltpu.VMEM((9, 2, sites), jnp.bfloat16),
            pltpu.VMEM((nsteps, rows, sites), jnp.bfloat16),
            pltpu.VMEM((more, 9, 2, sites), jnp.bfloat16),
            pltpu.VMEM((rows, sites), jnp.float32),
            pltpu.VMEM((rows, sites), jnp.float32),
            pltpu.SMEM(source_z.shape, jnp.int32),
            pltpu.SMEM(displacements.shape, jnp.int32),
            pltpu.SMEM(momenta.shape, jnp.int32),
            pltpu.SMEM(gamma_perm.shape, jnp.int32),
            pltpu.SMEM(gamma_phase.shape, jnp.int32),
            pltpu.VMEM((ngz, lane_rows, LANES), jnp.float32),
            pltpu.VMEM((nta, ngy, lane_rows, LANES), jnp.float32),
            dma((7,)), dma((nsteps,)), dma((nsteps,)), dma((more,)), dma((more,)),
            dma((ngz,)), dma((ngz,)), dma((nta * ngy,)), dma((nta * ngy,)),
        ],
        compiler_params=pltpu.CompilerParams(collective_id=0, has_side_effects=True),
    )(field, link, source_z, displacements, momenta, gamma_perm, gamma_phase)
    used = reduced.reshape(nta, lane_rows * LANES)[:, : ndisp * ng * np_ * 2]
    return jnp.swapaxes(used.reshape(nta, ndisp, ng, 2, np_), 3, 4)


def solution(mesh):
    placed = (
        P(None, None, None, None, "ta", "gz", "gy"),
        P(None, None, None, "ta", "gz", "gy"),
        P(),
        P(),
        P(),
        P(),
        P(),
    )
    ranks = tuple(mesh.shape[axis] for axis in ("ta", "gz", "gy"))
    return jax.shard_map(
        functools.partial(body, ranks), mesh=mesh, in_specs=placed, out_specs=P(), check_vma=False
    )
```

```python
import functools
import math

import jax
import jax.numpy as jnp
from jax import lax
from jax.experimental import pallas as pl
from jax.experimental.pallas import tpu as pltpu
from jax.sharding import PartitionSpec as P

MESH = pl.DeviceIdType.MESH
LANES = 128


def weights(lane_row, sizes, smem, place, scaling):
    ndisp, ng, np_, nz = sizes
    src, disp, mom, perm, phase = smem
    slice_at, depth_at = place
    nsteps = (ndisp - 1) // 2
    shape = (32, LANES)
    lane = lax.broadcasted_iota(jnp.int32, shape, 1) + lane_row * LANES
    row = lax.broadcasted_iota(jnp.int32, shape, 0)
    momentum = lane & (np_ - 1)
    out_part = (lane // np_) & 1
    gamma = (lane // (2 * np_)) & (ng - 1)
    entry = lane // (2 * np_ * ng)
    in_part = row // 16
    first = (row // 4) & 3
    second = row & 3
    reach = jnp.full(shape, 2 * nsteps + 1, jnp.int32)
    for j in range(ndisp):
        reach = jnp.where(entry == j, disp[j] - nsteps, reach)
    backward = reach < 0
    momenta = jnp.zeros(shape, jnp.int32)
    source = jnp.zeros(shape, jnp.int32)
    for p in range(np_):
        momenta = jnp.where(momentum == p, mom[p], momenta)
        source = jnp.where(momentum == p, src[slice_at, p], source)
    depth = depth_at - jnp.where(backward, reach, 0)
    turns = (momenta * (depth - source)).astype(jnp.float32) * (1.0 / nz)
    angle = (turns - jnp.floor(turns)) * (2.0 * math.pi)
    cosine = jnp.cos(angle)
    sine = jnp.sin(angle)
    sink = jnp.where(backward, second, first)
    other = jnp.where(backward, first, second)
    column = jnp.zeros(shape, jnp.int32)
    power = jnp.zeros(shape, jnp.int32)
    for g in range(ng):
        for s in range(4):
            here = (gamma == g) & (sink == s)
            column = jnp.where(here, perm[g, s], column)
            power = jnp.where(here, phase[g, s], power)
    quarter = power - out_part + jnp.where(backward, -in_part, in_part)
    quarter = quarter & 3
    value = jnp.where((quarter & 1) == 0, cosine, sine)
    value = jnp.where(quarter >= 2, -value, value)
    value = jnp.where((column == other) & (entry < ndisp), value * scaling, 0.0)
    return value, jnp.abs(reach)


def pair_sums(left, right, rows):
    half = rows // 2
    per = half // 4
    lefts = []
    turned = []
    rights = []
    for s in range(4):
        lefts.append(left[pl.ds(s, 2 * per, stride=4), :])
        rights.append(right[pl.ds(s, 2 * per, stride=4), :])
        turned.append(
            jnp.concatenate(
                [-left[pl.ds(half + s, per, stride=4), :], left[pl.ds(s, per, stride=4), :]],
                axis=0,
            )
        )
    out = []
    for group in (lefts, turned):
        for s in range(4):
            for u in range(4):
                product = (group[s] * rights[u]).reshape(2 * per // 8, 8, LANES)
                out.append(jnp.sum(jnp.sum(product, axis=0), axis=0, keepdims=True))
    stacked = jnp.concatenate(out, axis=0)
    return jnp.sum(stacked, axis=1, keepdims=True)


def kernel(
    sizes, scaling, ranks,
    prop, links, src_h, disp_h, mom_h, perm_h, phase_h,
    out,
    near, near_links, far, far_links, left, right,
    src, disp, mom, perm, phase,
    gathered, result,
    local_sem, s_send, s_recv, u_send, u_recv, a_send, a_recv,
):
    ndisp, ng, np_, nz = sizes
    nta, ngz, ngy = ranks
    nsteps = (ndisp - 1) // 2
    rows = near.shape[0]
    part_rows = rows // 2
    colour_rows = part_rows // 3
    lane_rows = gathered.shape[1]
    ta, gz, gy = lax.axis_index("ta"), lax.axis_index("gz"), lax.axis_index("gy")
    place = (ta * ngz + gz) * ngy + gy

    loads = [
        pltpu.make_async_copy(a, b, local_sem.at[i])
        for i, (a, b) in enumerate(
            [(prop, near), (links, near_links), (src_h, src), (disp_h, disp),
             (mom_h, mom), (perm_h, perm), (phase_h, phase)]
        )
    ]
    for load in loads:
        load.start()

    def peer(step):
        across = lax.rem(step // (ngy * ngz) + ta, nta)
        along = lax.rem(lax.rem(step, ngz) + gz, ngz)
        beside = lax.rem(lax.rem(step // ngz, ngy) + gy, ngy)
        return (across, along, beside)

    barrier = pltpu.get_barrier_semaphore()
    each(
        ranks,
        lambda step: pl.semaphore_signal(
            barrier, inc=1, device_id=peer(step), device_id_type=MESH
        ),
    )
    count = nta * ngz * ngy
    pl.semaphore_wait(barrier, count - 1)

    loads[0].wait()
    loads[1].wait()
    sends = []
    for k in range(1, nsteps + 1):
        target = (ta, lax.rem(gz + ngz - k, ngz), gy)
        sends.append(pltpu.make_async_remote_copy(
            src_ref=near, dst_ref=far.at[k - 1], send_sem=s_send.at[k - 1],
            recv_sem=s_recv.at[k - 1], device_id=target, device_id_type=MESH))
        sends[-1].start()
    link_sends = []
    for k in range(1, nsteps):
        target = (ta, lax.rem(gz + ngz - k, ngz), gy)
        link_sends.append(pltpu.make_async_remote_copy(
            src_ref=near_links, dst_ref=far_links.at[k - 1], send_sem=u_send.at[k - 1],
            recv_sem=u_recv.at[k - 1], device_id=target, device_id_type=MESH))
        link_sends[-1].start()

    for load in loads[2:]:
        load.wait()
    left[...] = near[...].astype(jnp.float32)
    sums = [pair_sums(left, left, rows)]
    tables = [
        weights(h, sizes, (src, disp, mom, perm, phase), (ta, gz), scaling)
        for h in range(lane_rows)
    ]

    def link_at(ref):
        return [
            [
                [jnp.broadcast_to(ref[3 * a + b, pl.ds(part, 1), :].astype(jnp.float32), (8, LANES))
                 for part in range(2)]
                for b in range(3)
            ]
            for a in range(3)
        ]

    wilson = None
    for k in range(1, nsteps + 1):
        if k == 1:
            wilson = link_at(near_links)
        else:
            link_sends[k - 2].wait_recv()
            step = link_at(far_links.at[k - 2])
            wilson = [
                [
                    [
                        sum(wilson[a][c][0] * step[c][b][0] - wilson[a][c][1] * step[c][b][1] for c in range(3)),
                        sum(wilson[a][c][0] * step[c][b][1] + wilson[a][c][1] * step[c][b][0] for c in range(3)),
                    ]
                    for b in range(3)
                ]
                for a in range(3)
            ]
        sends[k - 1].wait_recv()
        for chunk in range(colour_rows // 16):
            field = [
                [
                    far[k - 1, pl.ds(part * part_rows + b * colour_rows + chunk * 16, 16), :]
                    .astype(jnp.float32).reshape(2, 8, LANES)
                    for b in range(3)
                ]
                for part in range(2)
            ]
            for a in range(3):
                real = sum(wilson[a][b][0] * field[0][b] - wilson[a][b][1] * field[1][b] for b in range(3))
                imag = sum(wilson[a][b][0] * field[1][b] + wilson[a][b][1] * field[0][b] for b in range(3))
                at = a * colour_rows + chunk * 16
                right[pl.ds(at, 16), :] = real.reshape(16, LANES)
                right[pl.ds(part_rows + at, 16), :] = imag.reshape(16, LANES)
        sums.append(pair_sums(left, right, rows))

    for h in range(lane_rows):
        table, reach = tables[h]
        chosen = jnp.zeros(table.shape, jnp.float32)
        for k in range(nsteps + 1):
            chosen = jnp.where(reach == k, sums[k], chosen)
        gathered[place, pl.ds(h, 1), :] = jnp.sum(chosen * table, axis=0, keepdims=True)

    each(
        ranks,
        lambda step: pltpu.make_async_remote_copy(
            src_ref=gathered.at[place], dst_ref=gathered.at[place], send_sem=a_send.at[0],
            recv_sem=a_recv.at[0], device_id=peer(step), device_id_type=MESH).start(),
    )
    others = gathered.at[pl.ds(0, count - 1)]
    pltpu.make_async_copy(others, others, a_recv.at[0]).wait()
    for t in range(nta):
        block = gathered[pl.ds(t * ngz * ngy, ngz * ngy)]
        result[t] = jnp.sum(block, axis=0)
    done = pltpu.make_async_copy(result, out, local_sem.at[7])
    done.start()
    for copy in sends + link_sends:
        copy.wait_send()
    pltpu.make_async_copy(others, others, a_send.at[0]).wait()
    done.wait()


def each(ranks, act):
    nta, ngz, ngy = ranks
    count = nta * ngz * ngy
    if count > 64:
        lax.fori_loop(1, count, lambda step, carry: (act(step), carry)[1], 0)
        return
    for beside in (*range(1, ngy), 0):
        for across in range(nta - 1, -1, -1):
            for along in range(ngz):
                step = (across * ngy + beside) * ngz + along
                if step:
                    act(step)


def body(ranks, propagator, links, source_z, displacements, momenta, gamma_perm, gamma_phase):
    nta, ngz, ngy = ranks
    sites = propagator.shape[6]
    ndisp, np_, ng = displacements.shape[0], momenta.shape[0], gamma_perm.shape[0]
    nsteps = (ndisp - 1) // 2
    sizes = (ndisp, ng, np_, ngz)
    scaling = 1.0 / (24.0 * math.sqrt(sites * ngy * ngz))
    field = jnp.transpose(propagator, (0, 2, 3, 4, 5, 1, 6)).reshape(-1, sites)
    link = jnp.transpose(links, (1, 2, 3, 4, 0, 5)).reshape(9, 2, sites)
    rows = field.shape[0]
    lane_rows = -(-ndisp * ng * np_ * 2 // LANES)
    more = max(nsteps - 1, 1)
    dma = pltpu.SemaphoreType.DMA
    reduced = pl.pallas_call(
        functools.partial(kernel, sizes, scaling, ranks),
        out_shape=jax.ShapeDtypeStruct((nta, lane_rows, LANES), jnp.float32),
        in_specs=[pl.BlockSpec(memory_space=pltpu.HBM)] * 7,
        out_specs=pl.BlockSpec(memory_space=pl.ANY),
        scratch_shapes=[
            pltpu.VMEM((rows, sites), jnp.bfloat16),
            pltpu.VMEM((9, 2, sites), jnp.bfloat16),
            pltpu.VMEM((nsteps, rows, sites), jnp.bfloat16),
            pltpu.VMEM((more, 9, 2, sites), jnp.bfloat16),
            pltpu.VMEM((rows, sites), jnp.float32),
            pltpu.VMEM((rows, sites), jnp.float32),
            pltpu.SMEM(source_z.shape, jnp.int32),
            pltpu.SMEM(displacements.shape, jnp.int32),
            pltpu.SMEM(momenta.shape, jnp.int32),
            pltpu.SMEM(gamma_perm.shape, jnp.int32),
            pltpu.SMEM(gamma_phase.shape, jnp.int32),
            pltpu.VMEM((nta * ngz * ngy, lane_rows, LANES), jnp.float32),
            pltpu.VMEM((nta, lane_rows, LANES), jnp.float32),
            dma((8,)), dma((nsteps,)), dma((nsteps,)), dma((more,)), dma((more,)),
            dma((1,)), dma((1,)),
        ],
        compiler_params=pltpu.CompilerParams(collective_id=0, has_side_effects=True, vmem_limit_bytes=8 << 20),
    )(field, link, source_z, displacements, momenta, gamma_perm, gamma_phase)
    used = reduced.reshape(nta, lane_rows * LANES)[:, : ndisp * ng * np_ * 2]
    return jnp.swapaxes(used.reshape(nta, ndisp, ng, 2, np_), 3, 4)


def solution(mesh):
    placed = (
        P(None, None, None, None, "ta", "gz", "gy"),
        P(None, None, None, "ta", "gz", "gy"),
        P(),
        P(),
        P(),
        P(),
        P(),
    )
    ranks = tuple(mesh.shape[axis] for axis in ("ta", "gz", "gy"))
    return jax.shard_map(
        functools.partial(body, ranks), mesh=mesh, in_specs=placed, out_specs=P(), check_vma=False
    )
```

```python
import functools
import math

import jax
import jax.numpy as jnp
from jax import lax
from jax.experimental import pallas as pl
from jax.experimental.pallas import tpu as pltpu
from jax.sharding import PartitionSpec as P

MESH = pl.DeviceIdType.MESH
LANES = 128


def weights(lane_row, sizes, smem, place, scaling):
    ndisp, ng, np_, nz = sizes
    src, disp, mom, perm, phase = smem
    slice_at, depth_at = place
    nsteps = (ndisp - 1) // 2
    shape = (32, LANES)
    lane = lax.broadcasted_iota(jnp.int32, shape, 1) + lane_row * LANES
    row = lax.broadcasted_iota(jnp.int32, shape, 0)
    momentum = lane & (np_ - 1)
    out_part = (lane // np_) & 1
    gamma = (lane // (2 * np_)) & (ng - 1)
    entry = lane // (2 * np_ * ng)
    in_part = row // 16
    first = (row // 4) & 3
    second = row & 3
    reach = jnp.full(shape, 2 * nsteps + 1, jnp.int32)
    for j in range(ndisp):
        reach = jnp.where(entry == j, disp[j] - nsteps, reach)
    backward = reach < 0
    momenta = jnp.zeros(shape, jnp.int32)
    source = jnp.zeros(shape, jnp.int32)
    for p in range(np_):
        momenta = jnp.where(momentum == p, mom[p], momenta)
        source = jnp.where(momentum == p, src[slice_at, p], source)
    depth = depth_at - jnp.where(backward, reach, 0)
    turns = (momenta * (depth - source)).astype(jnp.float32) * (1.0 / nz)
    angle = (turns - jnp.floor(turns)) * (2.0 * math.pi)
    cosine = jnp.cos(angle)
    sine = jnp.sin(angle)
    sink = jnp.where(backward, second, first)
    other = jnp.where(backward, first, second)
    column = jnp.zeros(shape, jnp.int32)
    power = jnp.zeros(shape, jnp.int32)
    for g in range(ng):
        for s in range(4):
            here = (gamma == g) & (sink == s)
            column = jnp.where(here, perm[g, s], column)
            power = jnp.where(here, phase[g, s], power)
    quarter = power - out_part + jnp.where(backward, -in_part, in_part)
    quarter = quarter & 3
    value = jnp.where((quarter & 1) == 0, cosine, sine)
    value = jnp.where(quarter >= 2, -value, value)
    value = jnp.where((column == other) & (entry < ndisp), value * scaling, 0.0)
    return value, jnp.abs(reach)


def pair_sums(left, right, rows):
    half = rows // 2
    per = half // 4
    lefts = []
    turned = []
    rights = []
    for s in range(4):
        lefts.append(left[pl.ds(s, 2 * per, stride=4), :])
        rights.append(right[pl.ds(s, 2 * per, stride=4), :])
        turned.append(
            jnp.concatenate(
                [-left[pl.ds(half + s, per, stride=4), :], left[pl.ds(s, per, stride=4), :]],
                axis=0,
            )
        )
    out = []
    for group in (lefts, turned):
        for s in range(4):
            for u in range(4):
                product = (group[s] * rights[u]).reshape(2 * per // 8, 8, LANES)
                out.append(jnp.sum(jnp.sum(product, axis=0), axis=0, keepdims=True))
    stacked = jnp.concatenate(out, axis=0)
    return jnp.sum(stacked, axis=1, keepdims=True)


def kernel(
    sizes, scaling, ranks,
    prop, links, src_h, disp_h, mom_h, perm_h, phase_h,
    out,
    near, near_links, far, far_links, left, right,
    src, disp, mom, perm, phase,
    gathered,
    local_sem, s_send, s_recv, u_send, u_recv, a_send, a_recv,
):
    ndisp, ng, np_, nz = sizes
    nta, ngz, ngy = ranks
    nsteps = (ndisp - 1) // 2
    rows = near.shape[0]
    part_rows = rows // 2
    colour_rows = part_rows // 3
    lane_rows = gathered.shape[1]
    ta, gz, gy = lax.axis_index("ta"), lax.axis_index("gz"), lax.axis_index("gy")
    place = (ta * ngz + gz) * ngy + gy

    loads = [
        pltpu.make_async_copy(a, b, local_sem.at[i])
        for i, (a, b) in enumerate(
            [(prop, near), (links, near_links), (src_h, src), (disp_h, disp),
             (mom_h, mom), (perm_h, perm), (phase_h, phase)]
        )
    ]
    for load in loads:
        load.start()

    def peer(step):
        across = lax.rem(step // (ngy * ngz) + ta, nta)
        along = lax.rem(lax.rem(step, ngz) + gz, ngz)
        beside = lax.rem(lax.rem(step // ngz, ngy) + gy, ngy)
        return (across, along, beside)

    barrier = pltpu.get_barrier_semaphore()
    each(
        ranks,
        lambda step: pl.semaphore_signal(
            barrier, inc=1, device_id=peer(step), device_id_type=MESH
        ),
    )
    count = nta * ngz * ngy
    pl.semaphore_wait(barrier, count - 1)

    loads[0].wait()
    loads[1].wait()
    sends = []
    for k in range(1, nsteps + 1):
        target = (ta, lax.rem(gz + ngz - k, ngz), gy)
        sends.append(pltpu.make_async_remote_copy(
            src_ref=near, dst_ref=far.at[k - 1], send_sem=s_send.at[k - 1],
            recv_sem=s_recv.at[k - 1], device_id=target, device_id_type=MESH))
        sends[-1].start()
    link_sends = []
    for k in range(1, nsteps):
        target = (ta, lax.rem(gz + ngz - k, ngz), gy)
        link_sends.append(pltpu.make_async_remote_copy(
            src_ref=near_links, dst_ref=far_links.at[k - 1], send_sem=u_send.at[k - 1],
            recv_sem=u_recv.at[k - 1], device_id=target, device_id_type=MESH))
        link_sends[-1].start()

    for load in loads[2:]:
        load.wait()
    left[...] = near[...].astype(jnp.float32)
    sums = [pair_sums(left, left, rows)]
    tables = [
        weights(h, sizes, (src, disp, mom, perm, phase), (ta, gz), scaling)
        for h in range(lane_rows)
    ]

    def link_at(ref):
        return [
            [
                [jnp.broadcast_to(ref[3 * a + b, pl.ds(part, 1), :].astype(jnp.float32), (8, LANES))
                 for part in range(2)]
                for b in range(3)
            ]
            for a in range(3)
        ]

    wilson = None
    for k in range(1, nsteps + 1):
        if k == 1:
            wilson = link_at(near_links)
        else:
            link_sends[k - 2].wait_recv()
            step = link_at(far_links.at[k - 2])
            wilson = [
                [
                    [
                        sum(wilson[a][c][0] * step[c][b][0] - wilson[a][c][1] * step[c][b][1] for c in range(3)),
                        sum(wilson[a][c][0] * step[c][b][1] + wilson[a][c][1] * step[c][b][0] for c in range(3)),
                    ]
                    for b in range(3)
                ]
                for a in range(3)
            ]
        for chunk in range(colour_rows // 16):
            field = [
                [
                    near[pl.ds(part * part_rows + a * colour_rows + chunk * 16, 16), :]
                    .astype(jnp.float32).reshape(2, 8, LANES)
                    for a in range(3)
                ]
                for part in range(2)
            ]
            for b in range(3):
                real = sum(field[0][a] * wilson[a][b][0] + field[1][a] * wilson[a][b][1] for a in range(3))
                imag = sum(field[1][a] * wilson[a][b][0] - field[0][a] * wilson[a][b][1] for a in range(3))
                at = b * colour_rows + chunk * 16
                left[pl.ds(at, 16), :] = real.reshape(16, LANES)
                left[pl.ds(part_rows + at, 16), :] = imag.reshape(16, LANES)
        sends[k - 1].wait_recv()
        right[...] = far[k - 1].astype(jnp.float32)
        sums.append(pair_sums(left, right, rows))

    for h in range(lane_rows):
        table, reach = tables[h]
        chosen = jnp.zeros(table.shape, jnp.float32)
        for k in range(nsteps + 1):
            chosen = jnp.where(reach == k, sums[k], chosen)
        gathered[place, pl.ds(h, 1), :] = jnp.sum(chosen * table, axis=0, keepdims=True)

    each(
        ranks,
        lambda step: pltpu.make_async_remote_copy(
            src_ref=gathered.at[place], dst_ref=gathered.at[place], send_sem=a_send.at[0],
            recv_sem=a_recv.at[0], device_id=peer(step), device_id_type=MESH).start(),
    )
    others = gathered.at[pl.ds(0, count - 1)]
    pltpu.make_async_copy(others, others, a_recv.at[0]).wait()
    for t in range(nta):
        block = gathered[pl.ds(t * ngz * ngy, ngz * ngy)]
        out[t] = jnp.sum(block, axis=0)
    for copy in sends + link_sends:
        copy.wait_send()
    pltpu.make_async_copy(others, others, a_send.at[0]).wait()


def each(ranks, act):
    nta, ngz, ngy = ranks
    count = nta * ngz * ngy
    if count > 64:
        lax.fori_loop(1, count, lambda step, carry: (act(step), carry)[1], 0)
        return
    for beside in (*range(1, ngy), 0):
        for across in range(nta - 1, -1, -1):
            for along in range(ngz):
                step = (across * ngy + beside) * ngz + along
                if step:
                    act(step)


def body(ranks, propagator, links, source_z, displacements, momenta, gamma_perm, gamma_phase):
    nta, ngz, ngy = ranks
    sites = propagator.shape[6]
    ndisp, np_, ng = displacements.shape[0], momenta.shape[0], gamma_perm.shape[0]
    nsteps = (ndisp - 1) // 2
    sizes = (ndisp, ng, np_, ngz)
    scaling = 1.0 / (24.0 * math.sqrt(sites * ngy * ngz))
    field = jnp.transpose(propagator, (0, 2, 3, 4, 5, 1, 6)).reshape(-1, sites)
    link = jnp.transpose(links, (1, 2, 3, 4, 0, 5)).reshape(9, 2, sites)
    rows = field.shape[0]
    lane_rows = -(-ndisp * ng * np_ * 2 // LANES)
    more = max(nsteps - 1, 1)
    dma = pltpu.SemaphoreType.DMA
    reduced = pl.pallas_call(
        functools.partial(kernel, sizes, scaling, ranks),
        out_shape=pltpu.VMEM((nta, lane_rows, LANES), jnp.float32),
        in_specs=[pl.BlockSpec(memory_space=pltpu.HBM)] * 7,
        out_specs=pl.BlockSpec(memory_space=pltpu.VMEM),
        scratch_shapes=[
            pltpu.VMEM((rows, sites), jnp.bfloat16),
            pltpu.VMEM((9, 2, sites), jnp.bfloat16),
            pltpu.VMEM((nsteps, rows, sites), jnp.bfloat16),
            pltpu.VMEM((more, 9, 2, sites), jnp.bfloat16),
            pltpu.VMEM((rows, sites), jnp.float32),
            pltpu.VMEM((rows, sites), jnp.float32),
            pltpu.SMEM(source_z.shape, jnp.int32),
            pltpu.SMEM(displacements.shape, jnp.int32),
            pltpu.SMEM(momenta.shape, jnp.int32),
            pltpu.SMEM(gamma_perm.shape, jnp.int32),
            pltpu.SMEM(gamma_phase.shape, jnp.int32),
            pltpu.VMEM((nta * ngz * ngy, lane_rows, LANES), jnp.float32),
            dma((7,)), dma((nsteps,)), dma((nsteps,)), dma((more,)), dma((more,)),
            dma((1,)), dma((1,)),
        ],
        compiler_params=pltpu.CompilerParams(collective_id=0, has_side_effects=True),
    )(field, link, source_z, displacements, momenta, gamma_perm, gamma_phase)
    used = reduced.reshape(nta, lane_rows * LANES)[:, : ndisp * ng * np_ * 2]
    return jnp.swapaxes(used.reshape(nta, ndisp, ng, 2, np_), 3, 4)


def solution(mesh):
    placed = (
        P(None, None, None, None, "ta", "gz", "gy"),
        P(None, None, None, "ta", "gz", "gy"),
        P(),
        P(),
        P(),
        P(),
        P(),
    )
    ranks = tuple(mesh.shape[axis] for axis in ("ta", "gz", "gy"))
    return jax.shard_map(
        functools.partial(body, ranks), mesh=mesh, in_specs=placed, out_specs=P(), check_vma=False
    )
```

```python
import functools
import math

import jax
import jax.numpy as jnp
from jax import lax
from jax.experimental import pallas as pl
from jax.experimental.pallas import tpu as pltpu
from jax.sharding import PartitionSpec as P

MESH = pl.DeviceIdType.MESH
LANES = 128


def weights(lane_row, sizes, smem, place, scaling):
    ndisp, ng, np_, nz = sizes
    src, disp, mom, perm, phase = smem
    slice_at, depth_at = place
    nsteps = (ndisp - 1) // 2
    shape = (32, LANES)
    lane = lax.broadcasted_iota(jnp.int32, shape, 1) + lane_row * LANES
    row = lax.broadcasted_iota(jnp.int32, shape, 0)
    momentum = lane & (np_ - 1)
    out_part = (lane // np_) & 1
    gamma = (lane // (2 * np_)) & (ng - 1)
    entry = lane // (2 * np_ * ng)
    in_part = row // 16
    first = (row // 4) & 3
    second = row & 3
    reach = jnp.full(shape, 2 * nsteps + 1, jnp.int32)
    for j in range(ndisp):
        reach = jnp.where(entry == j, disp[j] - nsteps, reach)
    backward = reach < 0
    momenta = jnp.zeros(shape, jnp.int32)
    source = jnp.zeros(shape, jnp.int32)
    for p in range(np_):
        momenta = jnp.where(momentum == p, mom[p], momenta)
        source = jnp.where(momentum == p, src[slice_at, p], source)
    depth = depth_at - jnp.where(backward, reach, 0)
    turns = (momenta * (depth - source)).astype(jnp.float32) * (1.0 / nz)
    angle = (turns - jnp.floor(turns)) * (2.0 * math.pi)
    cosine = jnp.cos(angle)
    sine = jnp.sin(angle)
    sink = jnp.where(backward, second, first)
    other = jnp.where(backward, first, second)
    column = jnp.zeros(shape, jnp.int32)
    power = jnp.zeros(shape, jnp.int32)
    for g in range(ng):
        for s in range(4):
            here = (gamma == g) & (sink == s)
            column = jnp.where(here, perm[g, s], column)
            power = jnp.where(here, phase[g, s], power)
    quarter = power - out_part + jnp.where(backward, -in_part, in_part)
    quarter = quarter & 3
    value = jnp.where((quarter & 1) == 0, cosine, sine)
    value = jnp.where(quarter >= 2, -value, value)
    value = jnp.where((column == other) & (entry < ndisp), value * scaling, 0.0)
    return value, jnp.abs(reach)


def add_pairs(sums, left, turned, right, start, size):
    def rows(ref, s):
        return ref[pl.ds(start + s, size // 4, stride=4), :].reshape(-1, 8, LANES)

    rights = [rows(right, u) for u in range(4)]
    out = []
    for side in (left, turned):
        for s in range(4):
            own = rows(side, s)
            out += [jnp.sum(own * other, axis=0) for other in rights]
    return out if sums is None else [x + y for x, y in zip(sums, out)]


def site_sums(sums):
    stacked = jnp.concatenate([jnp.sum(x, axis=0, keepdims=True) for x in sums], axis=0)
    return jnp.sum(stacked, axis=1, keepdims=True)


def keep(left, turned, at, size, real, imag):
    real, imag = real.reshape(-1, LANES), imag.reshape(-1, LANES)
    left[pl.ds(at, size), :] = real
    left[pl.ds(at + size, size), :] = imag
    if turned is not None:
        turned[pl.ds(at, size), :] = -imag
        turned[pl.ds(at + size, size), :] = real


def kernel(
    sizes, scaling, ranks,
    prop, links, src_h, disp_h, mom_h, perm_h, phase_h,
    out,
    near, near_links, far, far_links, left, turned, right,
    src, disp, mom, perm, phase,
    gathered,
    local_sem, s_send, s_recv, u_send, u_recv, a_send, a_recv, line_sem, plane_sem,
):
    ndisp, ng, np_, nz = sizes
    nta, ngz, ngy = ranks
    nsteps = (ndisp - 1) // 2
    size = near.shape[2]
    lane_rows = gathered.shape[1]
    ta, gz, gy = lax.axis_index("ta"), lax.axis_index("gz"), lax.axis_index("gy")
    place = (ta * ngz + gz) * ngy + gy

    loads = [
        pltpu.make_async_copy(a, b, local_sem.at[i])
        for i, (a, b) in enumerate(
            [(prop.at[:, c], near.at[:, c]) for c in range(3)]
            + [(links, near_links), (src_h, src), (disp_h, disp),
               (mom_h, mom), (perm_h, perm), (phase_h, phase)]
        )
    ]
    for load in loads:
        load.start()

    def peer(step):
        across = lax.rem(step // (ngy * ngz) + ta, nta)
        along = lax.rem(lax.rem(step, ngz) + gz, ngz)
        beside = lax.rem(lax.rem(step // ngz, ngy) + gy, ngy)
        return (across, along, beside)

    depth_peers = [functools.partial(lambda d: (ta, lax.rem(gz + d, ngz), gy), d) for d in range(1, ngz)]
    beside_peers = [functools.partial(lambda d: (ta, gz, lax.rem(gy + d, ngy)), d) for d in range(1, ngy)]
    across_peers = [functools.partial(lambda d: (lax.rem(ta + d, nta), gz, gy), d) for d in range(1, nta)]

    def greet(semaphore, peers):
        for at in peers:
            pl.semaphore_signal(semaphore, inc=1, device_id=at(), device_id_type=MESH)

    count = nta * ngz * ngy
    barrier = pltpu.get_barrier_semaphore()
    greet(barrier, depth_peers + beside_peers + across_peers)
    pl.semaphore_wait(barrier, ngz + ngy + nta - 3)

    def target(k):
        return (ta, lax.rem(gz + ngz - k, ngz), gy)

    sends = [
        [
            pltpu.make_async_remote_copy(
                src_ref=near.at[:, c], dst_ref=far.at[k - 1, :, c], send_sem=s_send.at[k - 1, c],
                recv_sem=s_recv.at[k - 1, c], device_id=target(k), device_id_type=MESH)
            for c in range(3)
        ]
        for k in range(1, nsteps + 1)
    ]
    link_sends = [
        pltpu.make_async_remote_copy(
            src_ref=near_links, dst_ref=far_links.at[k - 1], send_sem=u_send.at[k - 1],
            recv_sem=u_recv.at[k - 1], device_id=target(k), device_id_type=MESH)
        for k in range(1, nsteps)
    ]
    for c in range(3):
        loads[c].wait()
        for copies in sends:
            copies[c].start()
    loads[3].wait()
    for copy in link_sends:
        copy.start()
    greet(line_sem.at[0], depth_peers)
    for load in loads[4:]:
        load.wait()

    sums = None
    for c in range(3):
        keep(left, turned, 2 * size * c, size, near[0, c].astype(jnp.float32), near[1, c].astype(jnp.float32))
        sums = add_pairs(sums, left, turned, left, 2 * size * c, 2 * size)
    totals = [site_sums(sums)]
    pl.semaphore_wait(line_sem.at[0], ngz - 1)
    greet(plane_sem.at[0], across_peers)
    tables = [
        weights(h, sizes, (src, disp, mom, perm, phase), (ta, gz), scaling)
        for h in range(lane_rows)
    ]

    def link_at(ref):
        return [
            [
                [jnp.broadcast_to(ref[3 * a + b, pl.ds(part, 1), :].astype(jnp.float32), (8, LANES))
                 for part in range(2)]
                for b in range(3)
            ]
            for a in range(3)
        ]

    wilson = None
    for k in range(1, nsteps + 1):
        if k == 1:
            wilson = link_at(near_links)
        else:
            link_sends[k - 2].wait_recv()
            step = link_at(far_links.at[k - 2])
            wilson = [
                [
                    [
                        sum(wilson[a][c][0] * step[c][b][0] - wilson[a][c][1] * step[c][b][1] for c in range(3)),
                        sum(wilson[a][c][0] * step[c][b][1] + wilson[a][c][1] * step[c][b][0] for c in range(3)),
                    ]
                    for b in range(3)
                ]
                for a in range(3)
            ]
        for chunk in range(size // 16):
            field = [
                [
                    near[part, a, pl.ds(chunk * 16, 16), :].astype(jnp.float32).reshape(2, 8, LANES)
                    for a in range(3)
                ]
                for part in range(2)
            ]
            for b in range(3):
                real = sum(field[0][a] * wilson[a][b][0] + field[1][a] * wilson[a][b][1] for a in range(3))
                imag = sum(field[1][a] * wilson[a][b][0] - field[0][a] * wilson[a][b][1] for a in range(3))
                real, imag = real.reshape(16, LANES), imag.reshape(16, LANES)
                at = 2 * size * b + chunk * 16
                left[pl.ds(at, 16), :] = real
                left[pl.ds(at + size, 16), :] = imag
                turned[pl.ds(at, 16), :] = -imag
                turned[pl.ds(at + size, 16), :] = real
        sums = None
        for c in range(3):
            sends[k - 1][c].wait_recv()
            keep(right, None, 2 * size * c, size,
                 far[k - 1, 0, c].astype(jnp.float32), far[k - 1, 1, c].astype(jnp.float32))
            sums = add_pairs(sums, left, turned, right, 2 * size * c, 2 * size)
        totals.append(site_sums(sums))

    for h in range(lane_rows):
        table, reach = tables[h]
        chosen = jnp.zeros(table.shape, jnp.float32)
        for k in range(nsteps + 1):
            chosen = jnp.where(reach == k, totals[k], chosen)
        gathered[place, pl.ds(h, 1), :] = jnp.sum(chosen * table, axis=0, keepdims=True)

    pl.semaphore_wait(plane_sem.at[0], nta - 1)
    each(
        ranks,
        lambda step: pltpu.make_async_remote_copy(
            src_ref=gathered.at[place], dst_ref=gathered.at[place], send_sem=a_send.at[0],
            recv_sem=a_recv.at[0], device_id=peer(step), device_id_type=MESH).start(),
    )
    others = gathered.at[pl.ds(0, count - 1)]
    pltpu.make_async_copy(others, others, a_recv.at[0]).wait()
    for t in range(nta):
        block = gathered[pl.ds(t * ngz * ngy, ngz * ngy)]
        out[t] = jnp.sum(block, axis=0)
    for copy in sum(sends, []) + link_sends:
        copy.wait_send()
    pltpu.make_async_copy(others, others, a_send.at[0]).wait()


def each(ranks, act):
    nta, ngz, ngy = ranks
    count = nta * ngz * ngy
    if count > 64:
        lax.fori_loop(1, count, lambda step, carry: (act(step), carry)[1], 0)
        return
    for beside in (*range(1, ngy), 0):
        for across in range(nta - 1, -1, -1):
            for along in range(ngz):
                step = (across * ngy + beside) * ngz + along
                if step:
                    act(step)


def body(ranks, propagator, links, source_z, displacements, momenta, gamma_perm, gamma_phase):
    nta, ngz, ngy = ranks
    sites = propagator.shape[6]
    ndisp, np_, ng = displacements.shape[0], momenta.shape[0], gamma_perm.shape[0]
    nsteps = (ndisp - 1) // 2
    sizes = (ndisp, ng, np_, ngz)
    scaling = 1.0 / (24.0 * math.sqrt(sites * ngy * ngz))
    field = jnp.transpose(propagator, (0, 2, 3, 4, 5, 1, 6)).reshape(2, 3, -1, sites)
    link = jnp.transpose(links, (1, 2, 3, 4, 0, 5)).reshape(9, 2, sites)
    size = field.shape[2]
    regular = pltpu.SemaphoreType.REGULAR
    lane_rows = -(-ndisp * ng * np_ * 2 // LANES)
    more = max(nsteps - 1, 1)
    dma = pltpu.SemaphoreType.DMA
    reduced = pl.pallas_call(
        functools.partial(kernel, sizes, scaling, ranks),
        out_shape=pltpu.VMEM((nta, lane_rows, LANES), jnp.float32),
        in_specs=[pl.BlockSpec(memory_space=pltpu.HBM)] * 7,
        out_specs=pl.BlockSpec(memory_space=pltpu.VMEM),
        scratch_shapes=[
            pltpu.VMEM((2, 3, size, sites), jnp.bfloat16),
            pltpu.VMEM((9, 2, sites), jnp.bfloat16),
            pltpu.VMEM((nsteps, 2, 3, size, sites), jnp.bfloat16),
            pltpu.VMEM((more, 9, 2, sites), jnp.bfloat16),
            pltpu.VMEM((6 * size, sites), jnp.float32),
            pltpu.VMEM((6 * size, sites), jnp.float32),
            pltpu.VMEM((6 * size, sites), jnp.float32),
            pltpu.SMEM(source_z.shape, jnp.int32),
            pltpu.SMEM(displacements.shape, jnp.int32),
            pltpu.SMEM(momenta.shape, jnp.int32),
            pltpu.SMEM(gamma_perm.shape, jnp.int32),
            pltpu.SMEM(gamma_phase.shape, jnp.int32),
            pltpu.VMEM((nta * ngz * ngy, lane_rows, LANES), jnp.float32),
            dma((9,)), dma((nsteps, 3)), dma((nsteps, 3)), dma((more,)), dma((more,)),
            dma((1,)), dma((1,)), regular((1,)), regular((1,)),
        ],
        compiler_params=pltpu.CompilerParams(collective_id=0, has_side_effects=True),
    )(field, link, source_z, displacements, momenta, gamma_perm, gamma_phase)
    used = reduced.reshape(nta, lane_rows * LANES)[:, : ndisp * ng * np_ * 2]
    return jnp.swapaxes(used.reshape(nta, ndisp, ng, 2, np_), 3, 4)


def solution(mesh):
    placed = (
        P(None, None, None, None, "ta", "gz", "gy"),
        P(None, None, None, "ta", "gz", "gy"),
        P(),
        P(),
        P(),
        P(),
        P(),
    )
    ranks = tuple(mesh.shape[axis] for axis in ("ta", "gz", "gy"))
    return jax.shard_map(
        functools.partial(body, ranks), mesh=mesh, in_specs=placed, out_specs=P(), check_vma=False
    )
```

```python
import functools
import math

import jax
import jax.numpy as jnp
from jax import lax
from jax.experimental import pallas as pl
from jax.experimental.pallas import tpu as pltpu
from jax.sharding import PartitionSpec as P

MESH = pl.DeviceIdType.MESH
LANES = 128


def weights(lane_row, sizes, smem, place, scaling):
    ndisp, ng, np_, nz = sizes
    src, disp, mom, perm, phase = smem
    slice_at, depth_at = place
    nsteps = (ndisp - 1) // 2
    shape = (32, LANES)
    lane = lax.broadcasted_iota(jnp.int32, shape, 1) + lane_row * LANES
    row = lax.broadcasted_iota(jnp.int32, shape, 0)
    momentum = lane & (np_ - 1)
    out_part = (lane // np_) & 1
    gamma = (lane // (2 * np_)) & (ng - 1)
    entry = lane // (2 * np_ * ng)
    in_part = row // 16
    first = (row // 4) & 3
    second = row & 3
    reach = jnp.full(shape, 2 * nsteps + 1, jnp.int32)
    for j in range(ndisp):
        reach = jnp.where(entry == j, disp[j] - nsteps, reach)
    backward = reach < 0
    momenta = jnp.zeros(shape, jnp.int32)
    source = jnp.zeros(shape, jnp.int32)
    for p in range(np_):
        momenta = jnp.where(momentum == p, mom[p], momenta)
        source = jnp.where(momentum == p, src[slice_at, p], source)
    depth = depth_at - jnp.where(backward, reach, 0)
    turns = (momenta * (depth - source)).astype(jnp.float32) * (1.0 / nz)
    angle = (turns - jnp.floor(turns)) * (2.0 * math.pi)
    cosine = jnp.cos(angle)
    sine = jnp.sin(angle)
    sink = jnp.where(backward, second, first)
    other = jnp.where(backward, first, second)
    column = jnp.zeros(shape, jnp.int32)
    power = jnp.zeros(shape, jnp.int32)
    for g in range(ng):
        for s in range(4):
            here = (gamma == g) & (sink == s)
            column = jnp.where(here, perm[g, s], column)
            power = jnp.where(here, phase[g, s], power)
    quarter = power - out_part + jnp.where(backward, -in_part, in_part)
    quarter = quarter & 3
    value = jnp.where((quarter & 1) == 0, cosine, sine)
    value = jnp.where(quarter >= 2, -value, value)
    value = jnp.where((column == other) & (entry < ndisp), value * scaling, 0.0)
    return value, jnp.abs(reach)


def add_pairs(sums, left, turned, right, start, size):
    def rows(ref, s):
        return ref[pl.ds(start + s, size // 4, stride=4), :].reshape(-1, 8, LANES)

    rights = [rows(right, u) for u in range(4)]
    out = []
    for side in (left, turned):
        for s in range(4):
            own = rows(side, s)
            out += [jnp.sum(own * other, axis=0) for other in rights]
    return out if sums is None else [x + y for x, y in zip(sums, out)]


def site_sums(sums):
    stacked = jnp.concatenate([jnp.sum(x, axis=0, keepdims=True) for x in sums], axis=0)
    return jnp.sum(stacked, axis=1, keepdims=True)


def keep(left, turned, at, size, real, imag):
    real, imag = real.reshape(-1, LANES), imag.reshape(-1, LANES)
    left[pl.ds(at, size), :] = real
    left[pl.ds(at + size, size), :] = imag
    if turned is not None:
        turned[pl.ds(at, size), :] = -imag
        turned[pl.ds(at + size, size), :] = real


def kernel(
    sizes, scaling, ranks,
    prop, links, src_h, disp_h, mom_h, perm_h, phase_h,
    out,
    near, near_links, far, far_links, left, turned, right,
    src, disp, mom, perm, phase,
    gathered,
    local_sem, s_send, s_recv, a_recv, line_sem, plane_sem, *link_sems,
):
    ndisp, ng, np_, nz = sizes
    nta, ngz, ngy = ranks
    nsteps = (ndisp - 1) // 2
    size = near.shape[2]
    lane_rows = gathered.shape[1]
    ta, gz, gy = lax.axis_index("ta"), lax.axis_index("gz"), lax.axis_index("gy")
    place = (ta * ngz + gz) * ngy + gy

    loads = [
        pltpu.make_async_copy(a, b, local_sem.at[i])
        for i, (a, b) in enumerate(
            [(prop, near), (links, near_links), (src_h, src), (disp_h, disp),
             (mom_h, mom), (perm_h, perm), (phase_h, phase)]
        )
    ]
    for load in loads:
        load.start()

    depth_peers = [functools.partial(lambda d: (ta, lax.rem(gz + d, ngz), gy), d) for d in range(1, ngz)]
    beside_peers = [functools.partial(lambda d: (ta, gz, lax.rem(gy + d, ngy)), d) for d in range(1, ngy)]
    across_peers = [functools.partial(lambda d: (lax.rem(ta + d, nta), gz, gy), d) for d in range(1, nta)]

    def greet(semaphore, peers):
        for at in peers:
            pl.semaphore_signal(semaphore, inc=1, device_id=at(), device_id_type=MESH)

    count = nta * ngz * ngy
    barrier = pltpu.get_barrier_semaphore()
    greet(barrier, depth_peers + beside_peers + across_peers)
    pl.semaphore_wait(barrier, ngz + ngy + nta - 3)

    def target(k):
        return (ta, lax.rem(gz + ngz - k, ngz), gy)

    sends = [
        [
            pltpu.make_async_remote_copy(
                src_ref=near.at[:, c], dst_ref=far.at[k - 1, :, c], send_sem=s_send.at[0],
                recv_sem=s_recv.at[k - 1, c], device_id=target(k), device_id_type=MESH)
            for c in range(3)
        ]
        for k in range(1, nsteps + 1)
    ]
    u_send, u_recv = link_sems if link_sems else (None, None)
    link_sends = [
        pltpu.make_async_remote_copy(
            src_ref=near_links, dst_ref=far_links.at[k - 1], send_sem=u_send.at[k - 1],
            recv_sem=u_recv.at[k - 1], device_id=target(k), device_id_type=MESH)
        for k in range(1, nsteps)
    ]
    loads[0].wait()
    for c in range(3):
        for copies in sends:
            copies[c].start()
    loads[1].wait()
    for copy in link_sends:
        copy.start()
    greet(line_sem.at[0], depth_peers)
    for load in loads[2:]:
        load.wait()

    sums = None
    for c in range(3):
        keep(left, turned, 2 * size * c, size, near[0, c].astype(jnp.float32), near[1, c].astype(jnp.float32))
        sums = add_pairs(sums, left, turned, left, 2 * size * c, 2 * size)
    totals = [site_sums(sums)]
    pl.semaphore_wait(line_sem.at[0], ngz - 1)
    greet(plane_sem.at[0], across_peers)
    tables = [
        weights(h, sizes, (src, disp, mom, perm, phase), (ta, gz), scaling)
        for h in range(lane_rows)
    ]

    def link_at(ref):
        return [
            [
                [jnp.broadcast_to(ref[3 * a + b, pl.ds(part, 1), :].astype(jnp.float32), (8, LANES))
                 for part in range(2)]
                for b in range(3)
            ]
            for a in range(3)
        ]

    wilson = None
    for k in range(1, nsteps + 1):
        if k == 1:
            wilson = link_at(near_links)
        else:
            link_sends[k - 2].wait_recv()
            step = link_at(far_links.at[k - 2])
            wilson = [
                [
                    [
                        sum(wilson[a][c][0] * step[c][b][0] - wilson[a][c][1] * step[c][b][1] for c in range(3)),
                        sum(wilson[a][c][0] * step[c][b][1] + wilson[a][c][1] * step[c][b][0] for c in range(3)),
                    ]
                    for b in range(3)
                ]
                for a in range(3)
            ]
        for chunk in range(size // 16):
            field = [
                [
                    near[part, a, pl.ds(chunk * 16, 16), :].astype(jnp.float32).reshape(2, 8, LANES)
                    for a in range(3)
                ]
                for part in range(2)
            ]
            for b in range(3):
                real = sum(field[0][a] * wilson[a][b][0] + field[1][a] * wilson[a][b][1] for a in range(3))
                imag = sum(field[1][a] * wilson[a][b][0] - field[0][a] * wilson[a][b][1] for a in range(3))
                real, imag = real.reshape(16, LANES), imag.reshape(16, LANES)
                at = 2 * size * b + chunk * 16
                left[pl.ds(at, 16), :] = real
                left[pl.ds(at + size, 16), :] = imag
                turned[pl.ds(at, 16), :] = -imag
                turned[pl.ds(at + size, 16), :] = real
        sums = None
        for c in range(3):
            sends[k - 1][c].wait_recv()
            keep(right, None, 2 * size * c, size,
                 far[k - 1, 0, c].astype(jnp.float32), far[k - 1, 1, c].astype(jnp.float32))
            sums = add_pairs(sums, left, turned, right, 2 * size * c, 2 * size)
        totals.append(site_sums(sums))

    for h in range(lane_rows):
        table, reach = tables[h]
        chosen = jnp.zeros(table.shape, jnp.float32)
        for k in range(nsteps + 1):
            chosen = jnp.where(reach == k, totals[k], chosen)
        gathered[place, pl.ds(h, 1), :] = jnp.sum(chosen * table, axis=0, keepdims=True)

    pl.semaphore_wait(plane_sem.at[0], nta - 1)
    pltpu.make_async_copy(far, far, s_send.at[0]).wait()
    each(
        ranks,
        place,
        lambda at: pltpu.make_async_remote_copy(
            src_ref=gathered.at[place], dst_ref=gathered.at[place], send_sem=s_send.at[0],
            recv_sem=a_recv.at[0], device_id=at, device_id_type=MESH).start(),
    )
    others = gathered.at[pl.ds(0, count - 1)]
    pltpu.make_async_copy(others, others, a_recv.at[0]).wait()
    for t in range(nta):
        block = gathered[pl.ds(t * ngz * ngy, ngz * ngy)]
        out[t] = jnp.sum(block, axis=0)
    for copy in link_sends:
        copy.wait_send()
    pltpu.make_async_copy(others, others, s_send.at[0]).wait()


def each(ranks, place, act):
    nta, ngz, ngy = ranks
    count = nta * ngz * ngy

    def one(step, along):
        beside = step // (nta * ngz)
        across = step // ngz % nta

        @pl.when(place != (across * ngz + along) * ngy + beside)
        def _():
            act((across, along, beside))

    if count > 64:
        lax.fori_loop(0, count, lambda step, carry: (one(step, step % ngz), carry)[1], 0)
        return
    for step in range(count):
        one(step, step % ngz)


def body(ranks, propagator, links, source_z, displacements, momenta, gamma_perm, gamma_phase):
    nta, ngz, ngy = ranks
    sites = propagator.shape[6]
    ndisp, np_, ng = displacements.shape[0], momenta.shape[0], gamma_perm.shape[0]
    nsteps = (ndisp - 1) // 2
    sizes = (ndisp, ng, np_, ngz)
    scaling = 1.0 / (24.0 * math.sqrt(sites * ngy * ngz))
    field = jnp.transpose(propagator, (0, 2, 3, 4, 5, 1, 6)).reshape(2, 3, -1, sites)
    link = jnp.transpose(links, (1, 2, 3, 4, 0, 5)).reshape(9, 2, sites)
    size = field.shape[2]
    regular = pltpu.SemaphoreType.REGULAR
    lane_rows = -(-ndisp * ng * np_ * 2 // LANES)
    more = max(nsteps - 1, 1)
    dma = pltpu.SemaphoreType.DMA
    reduced = pl.pallas_call(
        functools.partial(kernel, sizes, scaling, ranks),
        out_shape=pltpu.VMEM((nta, lane_rows, LANES), jnp.float32),
        in_specs=[pl.BlockSpec(memory_space=pltpu.HBM)] * 7,
        out_specs=pl.BlockSpec(memory_space=pltpu.VMEM),
        scratch_shapes=[
            pltpu.VMEM((2, 3, size, sites), jnp.bfloat16),
            pltpu.VMEM((9, 2, sites), jnp.bfloat16),
            pltpu.VMEM((nsteps, 2, 3, size, sites), jnp.bfloat16),
            pltpu.VMEM((more, 9, 2, sites), jnp.bfloat16),
            pltpu.VMEM((6 * size, sites), jnp.float32),
            pltpu.VMEM((6 * size, sites), jnp.float32),
            pltpu.VMEM((6 * size, sites), jnp.float32),
            pltpu.SMEM(source_z.shape, jnp.int32),
            pltpu.SMEM(displacements.shape, jnp.int32),
            pltpu.SMEM(momenta.shape, jnp.int32),
            pltpu.SMEM(gamma_perm.shape, jnp.int32),
            pltpu.SMEM(gamma_phase.shape, jnp.int32),
            pltpu.VMEM((nta * ngz * ngy, lane_rows, LANES), jnp.float32),
            dma((7,)), dma((1,)), dma((nsteps, 3)),
            dma((1,)), regular((1,)), regular((1,)),
        ] + [dma((nsteps - 1,))] * (2 if nsteps > 1 else 0),
        compiler_params=pltpu.CompilerParams(collective_id=0, has_side_effects=True),
    )(field, link, source_z, displacements, momenta, gamma_perm, gamma_phase)
    used = reduced.reshape(nta, lane_rows * LANES)[:, : ndisp * ng * np_ * 2]
    return jnp.swapaxes(used.reshape(nta, ndisp, ng, 2, np_), 3, 4)


def solution(mesh):
    placed = (
        P(None, None, None, None, "ta", "gz", "gy"),
        P(None, None, None, "ta", "gz", "gy"),
        P(),
        P(),
        P(),
        P(),
        P(),
    )
    ranks = tuple(mesh.shape[axis] for axis in ("ta", "gz", "gy"))
    return jax.shard_map(
        functools.partial(body, ranks), mesh=mesh, in_specs=placed, out_specs=P(), check_vma=False
    )
```
